32 devices in a mesh: orient: 8 (over z, y), dom: 4 (over x, core).
Axes of the slice: x: 2, y: 2, z: 4, core: 2. Of those that a mesh axis runs over, the one named last changes fastest.
Arguments:
- particles: bfloat16 [256, 8448], P(('dom', 'orient')), parts along dimension 0, may hold values from -12 to 12
- defocus: float32 [256], P(('dom', 'orient')), parts along dimension 0, may hold values from 10 to 60
- inv_noise: float32 [4224], replicated, may hold values from 0.5 to 2
- references: bfloat16 [13824, 8448], P(('dom', 'orient')), parts along dimension 0, may hold values from -0.25 to 0.25
- thresholds: int32 [256], P('dom'), parts along dimension 0, may hold values from 512 to 1023
- range_start: int32 [256], P('dom'), parts along dimension 0, may hold values from 0 to 3455
- range_len: int32 [256], P('dom'), parts along dimension 0, may hold values from 36 to 1727
Outputs:
- posterior: float32 [256, 3456], P('dom', 'orient'), parts along dimension 0
- cumulative: float32 [256, 3456], P('dom', 'orient'), parts along dimension 0
- log_evidence: float32 [256], P('dom'), parts along dimension 0
- kept_mass: float32 [256], P('dom'), parts along dimension 0
The draws below stay inside these ranges and needn't reach their ends.
There are 4 independent parts, one for each index of `dom`. The reference program is written for one: setup_inputs(seed, part) draws one part's arguments, and reference() takes and returns one part's arrays. A program takes and returns all parts, laid end to end along the dimension named above; an argument that names none is the same for every part. Nothing has to cross between parts.
All inputs are finite; a program needn't handle non-finite values.
Results may differ from the reference program's by a relative error of at most 0.0004.
The reference program's roundings to bfloat16 on the way (of `weighted`, `ctf_power` and `power`) count: a program that leaves them out, or rounds other values in their place, can miss the bound.
Values may be sent and summed in bfloat16 or wider, within the bound.
No kernel may reach another device: no remote copies, remote signals or barrier semaphores. Data moves between devices by JAX's collectives and lax.ppermute only.
A program may use at most 64 MiB of HBM per device.

```python
import math
import jax
import jax.numpy as jnp
from jax import lax

COEF = 4224
FEAT = 8448
ROT = 36
ORIENTS = 3456
P_SIZE = 64


def ctf_rows(defocus, coef):
    index = jnp.arange(coef, dtype=jnp.int32)
    row_pos = (index // 128).astype(jnp.float32)
    col_pos = (index % 128 - 64).astype(jnp.float32)
    freq = math.pi * (row_pos * row_pos + col_pos * col_pos) / 16384.0
    return -jnp.sin(defocus[:, None] * freq[None, :] + 0.07)


def strong_rows(key):
    return jax.random.randint(jax.random.fold_in(key, 15), (8,), 0, ORIENTS)


def ref_row(key, row, strong):
    row_key = jax.random.fold_in(jax.random.fold_in(key, 11), row)
    spread = jnp.exp(jax.random.uniform(jax.random.fold_in(row_key, 1), (), jnp.float32, math.log(0.7), math.log(1.4)))
    base = jax.random.normal(jax.random.fold_in(row_key, 2), (FEAT,), jnp.float32)
    is_strong = jnp.any(strong == row)
    amplitude = jnp.where(is_strong, 0.12, 0.02)
    return jnp.clip(amplitude * spread * base, -0.25, 0.25)


def defocus_of(key):
    return jax.random.uniform(jax.random.fold_in(key, 12), (P_SIZE,), jnp.float32, 20.0, 50.0)


def draw_references(key, part):
    strong = strong_rows(key)
    rows_all = jnp.arange(ORIENTS, dtype=jnp.int32)
    return jax.vmap(lambda row: ref_row(key, row, strong))(rows_all).astype(jnp.bfloat16)


def draw_defocus(key, part):
    return defocus_of(key)


def draw_particles(key, part):
    images = jax.random.normal(jax.random.fold_in(key, 13), (P_SIZE, FEAT), jnp.float32)
    strong = strong_rows(key)
    chosen = jax.random.randint(jax.random.fold_in(key, 14), (4,), 0, P_SIZE)
    targets = jax.random.uniform(jax.random.fold_in(key, 16), (4,), jnp.float32, 110.0, 250.0)
    first_rows = jax.vmap(lambda row: ref_row(key, row, strong))(strong[:4])
    second_rows = jax.vmap(lambda row: ref_row(key, row, strong))(strong[4:])
    ctf = ctf_rows(defocus_of(key)[chosen], FEAT // 2)
    ctf_both = jnp.concatenate([ctf, ctf], axis=1)
    gain_first = targets / (0.0078 * FEAT)
    gain_second = (targets - 2.0) / (0.0078 * FEAT)
    aligned = 0.3 * images[chosen] + ctf_both * (gain_first[:, None] * first_rows + gain_second[:, None] * second_rows)
    images = images.at[chosen].set(aligned)
    return jnp.clip(images, -12.0, 12.0).astype(jnp.bfloat16)


def place_ends(result, stream_key, low, largest):
    shape = result.shape
    spot = [jax.random.randint(jax.random.fold_in(stream_key, axis), (), 0, shape[axis]) for axis in range(len(shape))]
    result = result.at[tuple(spot)].set(low)
    longest = shape.index(max(shape))
    spot[longest] = (spot[longest] + 1) % shape[longest]
    return result.at[tuple(spot)].set(largest)


def setup_inputs(seed: int = 0, part: int = 0) -> dict:
    key_of = jax.random.split(jax.random.key(seed), 8)
    part_keys = jax.random.split(jax.random.fold_in(key_of[7], part), 8)
    particles = draw_particles(jax.random.fold_in(jax.random.fold_in(key_of[7], part), 71), part)
    defocus = draw_defocus(jax.random.fold_in(jax.random.fold_in(key_of[7], part), 71), part)
    inv_noise = jnp.clip(jnp.exp(jax.random.uniform(key_of[2], (COEF,), jnp.float32, math.log(0.5), math.log(2.0))), 0.5, 2.0)
    references = draw_references(jax.random.fold_in(jax.random.fold_in(key_of[7], part), 71), part)
    thresholds = place_ends(jax.random.randint(part_keys[4], (P_SIZE,), 512, 1024), jax.random.fold_in(part_keys[4], 1), 512, 1023).astype(jnp.int32)
    range_start = place_ends(jax.random.randint(part_keys[5], (P_SIZE,), 0, ORIENTS), jax.random.fold_in(part_keys[5], 1), 0, ORIENTS - 1).astype(jnp.int32)
    range_len = place_ends(jax.random.randint(part_keys[6], (P_SIZE,), ROT, ORIENTS // 2), jax.random.fold_in(part_keys[6], 1), ROT, (ORIENTS // 2) - 1).astype(jnp.int32)
    return dict(particles=particles, defocus=defocus, inv_noise=inv_noise, references=references, thresholds=thresholds, range_start=range_start, range_len=range_len)


def ctf_table(defocus, coef):
    index = jnp.arange(coef, dtype=jnp.int32)
    row_pos = (index // 128).astype(jnp.float32)
    col_pos = (index % 128 - 64).astype(jnp.float32)
    freq = math.pi * (row_pos * row_pos + col_pos * col_pos) / 16384.0
    return -jnp.sin(defocus[:, None] * freq[None, :] + 0.07)


def reference(particles, defocus, inv_noise, references, thresholds, range_start, range_len):
    coef = inv_noise.shape[0]
    ctf = ctf_table(defocus, coef)
    ctf_both = jnp.concatenate([ctf, ctf], axis=1)
    noise_both = jnp.concatenate([inv_noise, inv_noise])
    weighted = (particles.astype(jnp.float32) * ctf_both * noise_both[None, :]).astype(jnp.bfloat16)
    ctf_power = (ctf * ctf * inv_noise[None, :]).astype(jnp.bfloat16)
    real_part = references[:, :coef].astype(jnp.float32)
    imag_part = references[:, coef:].astype(jnp.float32)
    power = (real_part * real_part + imag_part * imag_part).astype(jnp.bfloat16)
    dims = (((1,), (1,)), ((), ()))
    scores = lax.dot_general(weighted, references, dims, preferred_element_type=jnp.float32)
    scores = scores - 0.5 * lax.dot_general(ctf_power, power, dims, preferred_element_type=jnp.float32)
    top_score = jnp.max(scores, axis=1)
    expon = jnp.exp(scores - top_score[:, None])
    total = jnp.sum(expon, axis=1)
    posterior = expon / total[:, None]
    cumulative = jnp.cumsum(posterior, axis=1)
    before = cumulative - posterior
    fraction = thresholds.astype(jnp.float32) / 1024.0
    kept = jnp.minimum(jnp.maximum(fraction[:, None] - before, 0.0), posterior)
    orient_ids = jnp.arange(ORIENTS, dtype=jnp.int32)
    inside = ((orient_ids[None, :] - range_start[:, None]) % ORIENTS) < range_len[:, None]
    kept_mass = jnp.sum(jnp.where(inside, kept, 0.0), axis=1)
    log_evidence = top_score + jnp.log(total)
    return posterior, cumulative, log_evidence, kept_mass
```

```python
import math

import jax
import jax.numpy as jnp
from jax import lax
from jax.experimental import pallas as pl
from jax.experimental.pallas import tpu as pltpu
from jax.sharding import PartitionSpec as P

LANES = 128
VMEM = pl.BlockSpec(memory_space=pltpu.VMEM)
SMEM = pl.BlockSpec(memory_space=pltpu.SMEM)
HBM = pl.BlockSpec(memory_space=pl.ANY)


def sine(x):
    turns = jnp.floor(x * (1.0 / math.pi) + 0.5)
    rest = x - turns * 3.1414794921875
    rest = rest - turns * 0.00011315941810607910156
    rest = rest - turns * 1.9841872589410058936e-09
    sq = rest * rest
    poly = sq * 2.6083159809786593541503e-06 - 0.0001981069071916863322258
    poly = poly * sq + 0.00833307858556509017944336
    poly = poly * sq - 0.166666597127914428710938
    value = rest + rest * (sq * poly)
    half = turns * 0.5
    odd = half - jnp.floor(half)
    return value * (1.0 - 4.0 * odd)


def column(row):
    size = row.shape[1]
    down = lax.broadcasted_iota(jnp.int32, (size, size), 0)
    across = lax.broadcasted_iota(jnp.int32, (size, size), 1)
    return jnp.sum(jnp.where(down == across, row, 0.0), axis=1, keepdims=True)


def pack_body(particles, defocus, out, sem):
    feat = particles.shape[1]
    copy = pltpu.make_async_copy(particles, out.at[:, pl.ds(0, feat)], sem)
    copy.start()
    value = column(defocus[...])
    high = value.astype(jnp.bfloat16).astype(jnp.float32)
    mid = (value - high).astype(jnp.bfloat16).astype(jnp.float32)
    low = value - high - mid
    lane = lax.broadcasted_iota(jnp.int32, (value.shape[0], LANES), 1)
    parts = jnp.where(lane == 0, high, jnp.where(lane == 1, mid, jnp.where(lane == 2, low, 0.0)))
    out[:, pl.ds(feat, LANES)] = parts.astype(jnp.bfloat16)
    copy.wait()


def power_body(references, out):
    rows, coef = out.shape
    for k in range(0, coef, LANES):
        real = references[:, pl.ds(k, LANES)].astype(jnp.float32)
        imag = references[:, pl.ds(coef + k, LANES)].astype(jnp.float32)
        out[:, pl.ds(k, LANES)] = (real * real + imag * imag).astype(jnp.bfloat16)


def score_body(*refs, count, all_orients):
    shard, start, length, noise, references, power = refs[:6]
    pieces = refs[6 : 6 + count]
    scores, stats = refs[6 + count : 8 + count]
    stage, focus, weighted, energy = refs[8 + count :]
    rows = pieces[0].shape[0]
    ori, feat = references.shape
    coef = feat // 2
    me = shard[0]
    places = [pl.ds(pl.multiple_of((me ^ b) * rows, rows), rows) for b in range(count)]
    for b in range(count):
        bits = pieces[b][:, pl.ds(feat, LANES)].astype(jnp.float32)
        value = bits[:, 0:1] + bits[:, 1:2] + bits[:, 2:3]
        focus[places[b], :] = jnp.broadcast_to(value, (rows, LANES))
    dims = (((1,), (1,)), ((), ()))
    total = None
    for first in range(0, coef, 2 * LANES):
        width = min(2 * LANES, coef - first)
        for k in range(first, first + width, LANES):
            at = pl.ds(k, LANES)
            also = pl.ds(coef + k, LANES)
            for b in range(count):
                stage[places[b], at] = pieces[b][:, at].astype(jnp.float32)
                stage[places[b], also] = pieces[b][:, also].astype(jnp.float32)
            row_pos = float(k // 128)
            col_pos = (lax.broadcasted_iota(jnp.int32, (1, LANES), 1) - 64).astype(jnp.float32)
            freq = math.pi * (row_pos * row_pos + col_pos * col_pos) / 16384.0
            ctf = -sine(focus[...] * freq + 0.07)
            noise_row = noise[:, at]
            weighted[:, at] = (stage[:, at] * ctf * noise_row).astype(jnp.bfloat16)
            weighted[:, also] = (stage[:, also] * ctf * noise_row).astype(jnp.bfloat16)
            energy[:, at] = (-0.5 * (ctf * ctf * noise_row).astype(jnp.bfloat16).astype(jnp.float32)).astype(jnp.bfloat16)
        for left, right, k in (
            (references, weighted, first),
            (references, weighted, coef + first),
            (power, energy, first),
        ):
            at = pl.ds(k, width)
            part = lax.dot_general(left[:, at], right[:, at], dims, preferred_element_type=jnp.float32)
            total = part if total is None else total + part
    scores[...] = total
    top = jnp.max(total, axis=0, keepdims=True)
    expon = jnp.exp(total - top)
    index = me * ori + lax.broadcasted_iota(jnp.int32, total.shape, 0)
    begin = start[...]
    end = begin + length[...]
    end = jnp.where(end > all_orients, end - all_orients, end)
    stats[0:1, :] = top
    stats[1:2, :] = jnp.sum(expon, axis=0, keepdims=True)
    stats[2:3, :] = jnp.sum(jnp.where(index < begin, expon, 0.0), axis=0, keepdims=True)
    stats[3:4, :] = jnp.sum(jnp.where(index < end, expon, 0.0), axis=0, keepdims=True)


def running_body(scores, stats, expon_out, running_out, expon_pad, running_pad):
    ori, count = scores.shape
    top = stats[0:1, :]
    carry = jnp.zeros((1, count), jnp.float32)
    sub = lax.broadcasted_iota(jnp.int32, (8, count), 0)
    for o in range(0, ori, 8):
        value = jnp.exp(scores[pl.ds(o, 8), :] - top)
        total = value
        for step in (1, 2, 4):
            total = total + jnp.where(sub >= step, pltpu.roll(total, step, 0), 0.0)
        total = total + carry
        carry = total[7:8, :]
        expon_pad[pl.ds(o, 8), pl.ds(0, count)] = value
        running_pad[pl.ds(o, 8), pl.ds(0, count)] = total
    for o in range(0, ori, LANES):
        width = min(LANES, ori - o)
        for c in range(0, count, LANES):
            high = min(LANES, count - c)
            for pad, out in ((expon_pad, expon_out), (running_pad, running_out)):
                block = pad[pl.ds(o, LANES), pl.ds(c, LANES)].T
                out[pl.ds(c, high), pl.ds(o, width)] = block[:high, :width]


def final_body(shard, near, far, thresholds, start, length, expon, running, *outs, all_orients):
    posterior, cumulative, evidence, mass = outs
    me = shard[0]
    half = near.shape[0] // 4
    tables = [near[pl.ds(4 * b, 4), :] for b in range(half)] + [far[pl.ds(4 * b, 4), :] for b in range(half)]
    top = tables[0][0:1, :]
    for table in tables[1:]:
        top = jnp.maximum(top, table[0:1, :])
    sums = jnp.zeros_like(tables[0])
    shifted = jnp.zeros_like(top)
    for b, table in enumerate(tables):
        scaled = table * jnp.exp(table[0:1, :] - top)
        sums = sums + scaled
        earlier = jnp.where((me ^ b) < me, 1.0, 0.0)
        shifted = shifted + earlier * scaled[1:2, :]
    total = sums[1:2, :]
    evidence[...] = top + jnp.log(total)
    fraction = thresholds[...].astype(jnp.float32) / 1024.0
    wraps = start[...] + length[...] > all_orients
    before = jnp.minimum(sums[2:3, :] / total, fraction)
    until = jnp.minimum(sums[3:4, :] / total, fraction)
    whole = jnp.where(wraps, jnp.minimum(1.0, fraction), 0.0)
    mass[...] = until - before + whole
    scale = column(jnp.exp(tables[0][0:1, :] - top) / total)
    shift = column(shifted / total)
    posterior[...] = expon[...] * scale
    cumulative[...] = running[...] * scale + shift


def on_device(particles, defocus, inv_noise, references, thresholds, range_start, range_len):
    n = lax.axis_size("orient")
    rows, feat = particles.shape
    coef = inv_noise.shape[0]
    ori = references.shape[0]
    count = n * rows
    all_orients = n * ori
    shard = lax.axis_index("orient").astype(jnp.int32).reshape(1)
    start = range_start.reshape(1, count)
    length = range_len.reshape(1, count)
    f32, bf16 = jnp.float32, jnp.bfloat16

    def swap(x, b):
        return lax.ppermute(x, "orient", [(i, i ^ b) for i in range(n)])

    packed = pl.pallas_call(
        pack_body,
        name="pack",
        out_shape=jax.ShapeDtypeStruct((rows, feat + LANES), bf16),
        in_specs=[HBM, VMEM],
        out_specs=VMEM,
        scratch_shapes=[pltpu.SemaphoreType.DMA],
    )(particles, defocus.reshape(1, rows))

    half = n // 2
    pieces = {0: packed, half: swap(packed, half)}
    for source in (0, half):
        for b in range(half - 1, 0, -1):
            pieces[source ^ b] = swap(pieces[source], b)

    power = pl.pallas_call(
        power_body,
        name="power",
        out_shape=jax.ShapeDtypeStruct((ori, coef), bf16),
        in_specs=[VMEM],
        out_specs=VMEM,
    )(references)

    scores, stats = pl.pallas_call(
        lambda *refs: score_body(*refs, count=n, all_orients=all_orients),
        name="score",
        out_shape=(jax.ShapeDtypeStruct((ori, count), f32), jax.ShapeDtypeStruct((4, count), f32)),
        in_specs=[SMEM] + [VMEM] * (5 + n),
        out_specs=(VMEM, VMEM),
        scratch_shapes=[
            pltpu.VMEM((count, feat), f32),
            pltpu.VMEM((count, LANES), f32),
            pltpu.VMEM((count, feat), bf16),
            pltpu.VMEM((count, coef), bf16),
        ],
    )(shard, start, length, inv_noise.reshape(1, coef), references, power, *[pieces[b] for b in range(n)])

    near = stats
    b = 1
    while b < half:
        near = jnp.concatenate([near, swap(near, b)], axis=0)
        b *= 2
    far = swap(near, half)

    pad_ori = -(-ori // LANES) * LANES
    pad_count = -(-count // LANES) * LANES
    expon, running = pl.pallas_call(
        running_body,
        name="running",
        out_shape=(jax.ShapeDtypeStruct((count, ori), f32),) * 2,
        in_specs=[VMEM, VMEM],
        out_specs=(VMEM, VMEM),
        scratch_shapes=[pltpu.VMEM((pad_ori, pad_count), f32)] * 2,
    )(scores, stats)

    posterior, cumulative, evidence, mass = pl.pallas_call(
        lambda *refs: final_body(*refs, all_orients=all_orients),
        name="final",
        out_shape=(jax.ShapeDtypeStruct((count, ori), f32),) * 2 + (jax.ShapeDtypeStruct((1, count), f32),) * 2,
        in_specs=[SMEM] + [VMEM] * 7,
        out_specs=(VMEM,) * 4,
    )(shard, near, far, thresholds.reshape(1, count), start, length, expon, running)
    return posterior, cumulative, evidence.reshape(count), mass.reshape(count)


def solution(mesh):
    return jax.shard_map(
        on_device,
        mesh=mesh,
        in_specs=(
            P(("dom", "orient"), None),
            P(("dom", "orient")),
            P(),
            P(("dom", "orient"), None),
            P("dom"),
            P("dom"),
            P("dom"),
        ),
        out_specs=(P("dom", "orient"), P("dom", "orient"), P("dom"), P("dom")),
        check_vma=False,
    )
```

```python
import math

import jax
import jax.numpy as jnp
from jax import lax
from jax.experimental import pallas as pl
from jax.experimental.pallas import tpu as pltpu
from jax.sharding import PartitionSpec as P

LANES = 128
VMEM = pl.BlockSpec(memory_space=pltpu.VMEM)
SMEM = pl.BlockSpec(memory_space=pltpu.SMEM)
HBM = pl.BlockSpec(memory_space=pltpu.HBM)


def sine(x):
    turns = jnp.floor(x * (1.0 / math.pi) + 0.5)
    rest = x - turns * 3.1414794921875
    rest = rest - turns * 0.00011315941810607910156
    rest = rest - turns * 1.9841872589410058936e-09
    sq = rest * rest
    poly = sq * 2.6083159809786593541503e-06 - 0.0001981069071916863322258
    poly = poly * sq + 0.00833307858556509017944336
    poly = poly * sq - 0.166666597127914428710938
    value = rest + rest * (sq * poly)
    half = turns * 0.5
    odd = half - jnp.floor(half)
    return value * (1.0 - 4.0 * odd)


def column(row):
    size = row.shape[1]
    down = lax.broadcasted_iota(jnp.int32, (size, size), 0)
    across = lax.broadcasted_iota(jnp.int32, (size, size), 1)
    return jnp.sum(jnp.where(down == across, row, 0.0), axis=1, keepdims=True)


def pack_body(particles, defocus, out, row, sems):
    feat = particles.shape[1]
    copy = pltpu.make_async_copy(particles, out.at[:, pl.ds(0, feat)], sems.at[0])
    fetch = pltpu.make_async_copy(defocus, row, sems.at[1])
    copy.start()
    fetch.start()
    fetch.wait()
    value = column(row[...])
    high = value.astype(jnp.bfloat16).astype(jnp.float32)
    mid = (value - high).astype(jnp.bfloat16).astype(jnp.float32)
    low = value - high - mid
    lane = lax.broadcasted_iota(jnp.int32, (value.shape[0], LANES), 1)
    parts = jnp.where(lane == 0, high, jnp.where(lane == 1, mid, jnp.where(lane == 2, low, 0.0)))
    out[:, pl.ds(feat, LANES)] = parts.astype(jnp.bfloat16)
    copy.wait()


def power_body(references, local, out, sems):
    rows, coef = out.shape
    step = -(-rows // (8 * sems.shape[0])) * 8
    spans = [pl.ds(r, min(step, rows - r)) for r in range(0, rows, step)]
    copies = [pltpu.make_async_copy(references.at[span], local.at[span], sems.at[i]) for i, span in enumerate(spans)]
    for copy in copies:
        copy.start()
    for span, copy in zip(spans, copies):
        copy.wait()
        for k in range(0, coef, LANES):
            real = local[span, pl.ds(k, LANES)].astype(jnp.float32)
            imag = local[span, pl.ds(coef + k, LANES)].astype(jnp.float32)
            out[span, pl.ds(k, LANES)] = (real * real + imag * imag).astype(jnp.bfloat16)


def score_body(*refs, pieces, all_orients):
    shard, start, length, noise, references, power = refs[:6]
    packed = refs[6 : 6 + pieces]
    scores, stats = refs[6 + pieces : 8 + pieces]
    stage, focus, weighted, energy = refs[8 + pieces :]
    rows = packed[0].shape[0]
    count = focus.shape[0]
    ori, feat = references.shape
    coef = feat // 2
    me = shard[0]
    places = [pl.ds(pl.multiple_of((me ^ b) * rows, rows), rows) if pieces > 1 else pl.ds(0, rows) for b in range(pieces)]
    for b in range(pieces):
        bits = packed[b][:, pl.ds(feat, LANES)].astype(jnp.float32)
        value = bits[:, 0:1] + bits[:, 1:2] + bits[:, 2:3]
        focus[places[b], :] = jnp.broadcast_to(value, (rows, LANES))
    dims = (((1,), (1,)), ((), ()))
    col_pos = (lax.broadcasted_iota(jnp.int32, (1, LANES), 1) - 64).astype(jnp.float32)

    def images(at):
        if pieces == 1:
            return packed[0][:, at].astype(jnp.float32)
        for b in range(pieces):
            stage[places[b], at] = packed[b][:, at].astype(jnp.float32)
        return stage[:, at]

    def chunk(first, width, total):
        for k in range(0, width, LANES):
            at = pl.ds(first + k, LANES)
            also = pl.ds(coef + first + k, LANES)
            row_pos = jnp.asarray((first + k) // 128).astype(jnp.float32)
            freq = math.pi * (row_pos * row_pos + col_pos * col_pos) / 16384.0
            ctf = -sine(focus[...] * freq + 0.07)
            noise_row = noise[at].reshape(1, LANES)
            weighted[:, at] = (images(at) * ctf * noise_row).astype(jnp.bfloat16)
            weighted[:, also] = (images(also) * ctf * noise_row).astype(jnp.bfloat16)
            energy[:, at] = (-0.5 * (ctf * ctf * noise_row).astype(jnp.bfloat16).astype(jnp.float32)).astype(jnp.bfloat16)
        for left, right, k in (
            (references, weighted, first),
            (references, weighted, coef + first),
            (power, energy, first),
        ):
            at = pl.ds(k, width)
            total = total + lax.dot_general(left[:, at], right[:, at], dims, preferred_element_type=jnp.float32)
        return total

    step = 2 * LANES
    total = jnp.zeros((ori, count), jnp.float32)
    if pieces > 1:
        for first in range(0, coef - coef % step, step):
            total = chunk(first, step, total)
    else:
        scores[...] = total

        @pl.loop(0, coef // step)
        def _(i):
            scores[...] = chunk(pl.multiple_of(i * step, step), step, scores[...])

        total = scores[...]
    if coef % step:
        total = chunk(coef - coef % step, coef % step, total)
    scores[...] = total
    top = jnp.max(total, axis=0, keepdims=True)
    expon = jnp.exp(total - top)
    index = me * ori + lax.broadcasted_iota(jnp.int32, total.shape, 0)
    begin = start[...]
    end = begin + length[...]
    end = jnp.where(end > all_orients, end - all_orients, end)
    stats[0:1, :] = top
    stats[1:2, :] = jnp.sum(expon, axis=0, keepdims=True)
    stats[2:3, :] = jnp.sum(jnp.where(index < begin, expon, 0.0), axis=0, keepdims=True)
    stats[3:4, :] = jnp.sum(jnp.where(index < end, expon, 0.0), axis=0, keepdims=True)


def running_body(scores, stats, expon_out, running_out, expon_pad, running_pad):
    ori, count = scores.shape
    top = stats[0:1, :]
    carry = jnp.zeros((1, count), jnp.float32)
    sub = lax.broadcasted_iota(jnp.int32, (8, count), 0)
    for o in range(0, ori, 8):
        value = jnp.exp(scores[pl.ds(o, 8), :] - top)
        total = value
        for step in (1, 2, 4):
            total = total + jnp.where(sub >= step, pltpu.roll(total, step, 0), 0.0)
        total = total + carry
        carry = total[7:8, :]
        expon_pad[pl.ds(o, 8), pl.ds(0, count)] = value
        running_pad[pl.ds(o, 8), pl.ds(0, count)] = total
    for o in range(0, ori, LANES):
        width = min(LANES, ori - o)
        for c in range(0, count, LANES):
            high = min(LANES, count - c)
            for pad, out in ((expon_pad, expon_out), (running_pad, running_out)):
                block = pad[pl.ds(o, LANES), pl.ds(c, LANES)].T
                out[pl.ds(c, high), pl.ds(o, width)] = block[:high, :width]


def final_body(shard, near, far, thresholds, start, length, expon, running, *outs, all_orients):
    posterior, cumulative, evidence, mass = outs
    me = shard[0]
    half = near.shape[0] // 4
    tables = [near[pl.ds(4 * b, 4), :] for b in range(half)] + [far[pl.ds(4 * b, 4), :] for b in range(half)]
    top = tables[0][0:1, :]
    for table in tables[1:]:
        top = jnp.maximum(top, table[0:1, :])
    sums = jnp.zeros_like(tables[0])
    shifted = jnp.zeros_like(top)
    for b, table in enumerate(tables):
        scaled = table * jnp.exp(table[0:1, :] - top)
        sums = sums + scaled
        earlier = jnp.where((me ^ b) < me, 1.0, 0.0)
        shifted = shifted + earlier * scaled[1:2, :]
    total = sums[1:2, :]
    evidence[...] = top + jnp.log(total)
    fraction = thresholds[...].astype(jnp.float32) / 1024.0
    wraps = start[...] + length[...] > all_orients
    before = jnp.minimum(sums[2:3, :] / total, fraction)
    until = jnp.minimum(sums[3:4, :] / total, fraction)
    whole = jnp.where(wraps, jnp.minimum(1.0, fraction), 0.0)
    mass[...] = until - before + whole
    scale = column(jnp.exp(tables[0][0:1, :] - top) / total)
    shift = column(shifted / total)
    posterior[...] = expon[...] * scale
    cumulative[...] = running[...] * scale + shift


def call(body, name, limit, **kwargs):
    params = pltpu.CompilerParams(vmem_limit_bytes=limit)
    return pl.pallas_call(body, name=name, compiler_params=params, **kwargs)


def in_vmem(x):
    return pltpu.with_memory_space_constraint(x, pltpu.VMEM)


def in_hbm(x):
    return pltpu.with_memory_space_constraint(x, pltpu.HBM)


def on_device(particles, defocus, inv_noise, references, thresholds, range_start, range_len):
    n = lax.axis_size("orient")
    rows, feat = particles.shape
    coef = inv_noise.shape[0]
    ori = references.shape[0]
    count = n * rows
    all_orients = n * ori
    shard = lax.axis_index("orient").astype(jnp.int32).reshape(1)
    start = in_vmem(range_start.reshape(1, count))
    length = in_vmem(range_len.reshape(1, count))
    fraction = in_vmem(thresholds.reshape(1, count))
    f32, bf16 = jnp.float32, jnp.bfloat16

    def swap(x, b):
        return lax.ppermute(x, "orient", [(i, i ^ b) for i in range(n)])

    packed = call(
        pack_body,
        "pack",
        2**21,
        out_shape=pltpu.VMEM((rows, feat + LANES), bf16),
        in_specs=[HBM, HBM],
        out_specs=VMEM,
        scratch_shapes=[pltpu.VMEM((1, rows), f32), pltpu.SemaphoreType.DMA((2,))],
    )(in_hbm(particles), in_hbm(defocus.reshape(1, rows)))

    half = n // 2
    if n <= 8:
        pieces = {0: packed, half: swap(packed, half)}
        for source in (0, half):
            for b in range(half - 1, 0, -1):
                pieces[source ^ b] = swap(pieces[source], b)
        pieces = [pieces[b] for b in range(n)]
    else:
        pieces = [lax.all_gather(packed, "orient", axis=0, tiled=True)]

    local, power = call(
        power_body,
        "power",
        2**21,
        out_shape=(pltpu.VMEM((ori, feat), bf16), pltpu.VMEM((ori, coef), bf16)),
        in_specs=[HBM],
        out_specs=(VMEM, VMEM),
        scratch_shapes=[pltpu.SemaphoreType.DMA((9,))],
    )(in_hbm(references))

    room = 2**22 + 4 * count * (feat + LANES) + 3 * count * feat
    scores, stats = call(
        lambda *refs: score_body(*refs, pieces=len(pieces), all_orients=all_orients),
        "score",
        room,
        out_shape=(pltpu.VMEM((ori, count), f32), pltpu.VMEM((4, count), f32)),
        in_specs=[SMEM] + [VMEM] * (5 + len(pieces)),
        out_specs=(VMEM, VMEM),
        scratch_shapes=[
            pltpu.VMEM((count, feat) if len(pieces) > 1 else (8, LANES), f32),
            pltpu.VMEM((count, LANES), f32),
            pltpu.VMEM((count, feat), bf16),
            pltpu.VMEM((count, coef), bf16),
        ],
    )(shard, start, length, in_vmem(inv_noise), in_vmem(local), in_vmem(power), *[in_vmem(p) for p in pieces])

    near = stats
    b = 1
    while b < half:
        near = jnp.concatenate([near, swap(near, b)], axis=0)
        b *= 2
    far = swap(near, half)

    pad_ori = -(-ori // LANES) * LANES
    pad_count = -(-count // LANES) * LANES
    expon, running = call(
        running_body,
        "running",
        2**23,
        out_shape=(pltpu.VMEM((count, ori), f32),) * 2,
        in_specs=[VMEM, VMEM],
        out_specs=(VMEM, VMEM),
        scratch_shapes=[pltpu.VMEM((pad_ori, pad_count), f32)] * 2,
    )(in_vmem(scores), in_vmem(stats))

    posterior, cumulative, evidence, mass = call(
        lambda *refs: final_body(*refs, all_orients=all_orients),
        "final",
        2**23,
        out_shape=(jax.ShapeDtypeStruct((count, ori), f32),) * 2 + (jax.ShapeDtypeStruct((1, count), f32),) * 2,
        in_specs=[SMEM] + [VMEM] * 7,
        out_specs=(VMEM,) * 4,
    )(shard, in_vmem(near), in_vmem(far), fraction, start, length, in_vmem(expon), in_vmem(running))
    return posterior, cumulative, evidence.reshape(count), mass.reshape(count)


def solution(mesh):
    return jax.shard_map(
        on_device,
        mesh=mesh,
        in_specs=(
            P(("dom", "orient"), None),
            P(("dom", "orient")),
            P(),
            P(("dom", "orient"), None),
            P("dom"),
            P("dom"),
            P("dom"),
        ),
        out_specs=(P("dom", "orient"), P("dom", "orient"), P("dom"), P("dom")),
        check_vma=False,
    )
```

```python
import math

import jax
import jax.numpy as jnp
from jax import lax
from jax.experimental import pallas as pl
from jax.experimental.pallas import tpu as pltpu
from jax.sharding import PartitionSpec as P


LANES = 128
ROUTE = ((0, 4, 4), (0, 3, 3), (0, 2, 2), (0, 1, 1), (1, 3, 3), (1, 2, 2), (1, 1, 1))
VMEM = pl.BlockSpec(memory_space=pltpu.VMEM)
HBM = pl.BlockSpec(memory_space=pltpu.HBM)


def sine(x):
    turns = jnp.floor(x * (1.0 / math.pi) + 0.5)
    rest = x - turns * 3.1414794921875
    rest = rest - turns * 0.00011315941810607910156
    rest = rest - turns * 1.9841872589410058936e-09
    sq = rest * rest
    poly = sq * 2.6083159809786593541503e-06 - 0.0001981069071916863322258
    poly = poly * sq + 0.00833307858556509017944336
    poly = poly * sq - 0.166666597127914428710938
    value = rest + rest * (sq * poly)
    half = turns * 0.5
    odd = half - jnp.floor(half)
    return value * (1.0 - 4.0 * odd)


def column(row):
    size = row.shape[1]
    down = lax.broadcasted_iota(jnp.int32, (size, size), 0)
    across = lax.broadcasted_iota(jnp.int32, (size, size), 1)
    return jnp.sum(jnp.where(down == across, row, 0.0), axis=1, keepdims=True)


def pack_body(particles, defocus, out, row, sems):
    feat = particles.shape[1]
    copy = pltpu.make_async_copy(particles, out.at[:, pl.ds(0, feat)], sems.at[0])
    fetch = pltpu.make_async_copy(defocus, row, sems.at[1])
    copy.start()
    fetch.start()
    fetch.wait()
    value = column(row[...])
    high = value.astype(jnp.bfloat16).astype(jnp.float32)
    mid = (value - high).astype(jnp.bfloat16).astype(jnp.float32)
    low = value - high - mid
    lane = lax.broadcasted_iota(jnp.int32, (value.shape[0], LANES), 1)
    parts = jnp.where(lane == 0, high, jnp.where(lane == 1, mid, jnp.where(lane == 2, low, 0.0)))
    out[:, pl.ds(feat, LANES)] = parts.astype(jnp.bfloat16)
    copy.wait()


def power_body(references, local, out, sems):
    rows, coef = out.shape
    step = -(-rows // (8 * sems.shape[0])) * 8
    spans = [pl.ds(r, min(step, rows - r)) for r in range(0, rows, step)]
    copies = [pltpu.make_async_copy(references.at[span], local.at[span], sems.at[i]) for i, span in enumerate(spans)]
    for copy in copies:
        copy.start()
    for span, copy in zip(spans, copies):
        copy.wait()
        for k in range(0, coef, LANES):
            real = local[span, pl.ds(k, LANES)].astype(jnp.float32)
            imag = local[span, pl.ds(coef + k, LANES)].astype(jnp.float32)
            out[span, pl.ds(k, LANES)] = (real * real + imag * imag).astype(jnp.bfloat16)


def score_body(*refs, pieces, offsets, all_orients):
    start, length, noise, references, power = refs[:5]
    packed = refs[5 : 5 + pieces]
    scores, stats = refs[5 + pieces : 7 + pieces]
    stage, focus, weighted, energy = refs[7 + pieces :]
    rows = packed[0].shape[0]
    count = focus.shape[0]
    ori, feat = references.shape
    coef = feat // 2
    me = lax.axis_index("orient")
    side = lax.axis_index("dom") & 1
    places = [pl.ds(0, rows)]
    if pieces > 1:
        owners = [me ^ (even + side * (odd - even)) if even != odd else me ^ even for even, odd in offsets]
        places = [pl.ds(pl.multiple_of(owner * rows, rows), rows) for owner in owners]
    for b in range(pieces):
        bits = packed[b][:, pl.ds(feat, LANES)].astype(jnp.float32)
        value = bits[:, 0:1] + bits[:, 1:2] + bits[:, 2:3]
        focus[places[b], :] = jnp.broadcast_to(value, (rows, LANES))
    dims = (((1,), (1,)), ((), ()))
    col_pos = (lax.broadcasted_iota(jnp.int32, (1, LANES), 1) - 64).astype(jnp.float32)

    def images(at):
        if pieces == 1:
            return packed[0][:, at].astype(jnp.float32)
        for b in range(pieces):
            stage[places[b], at] = packed[b][:, at].astype(jnp.float32)
        return stage[:, at]

    def chunk(first, width, total):
        for k in range(0, width, LANES):
            at = pl.ds(first + k, LANES)
            also = pl.ds(coef + first + k, LANES)
            row_pos = jnp.asarray((first + k) // 128).astype(jnp.float32)
            freq = math.pi * (row_pos * row_pos + col_pos * col_pos) / 16384.0
            ctf = -sine(focus[...] * freq + 0.07)
            noise_row = noise[at].reshape(1, LANES)
            weighted[:, at] = (images(at) * ctf * noise_row).astype(jnp.bfloat16)
            weighted[:, also] = (images(also) * ctf * noise_row).astype(jnp.bfloat16)
            energy[:, at] = (-0.5 * (ctf * ctf * noise_row).astype(jnp.bfloat16).astype(jnp.float32)).astype(jnp.bfloat16)
        for left, right, k in (
            (references, weighted, first),
            (references, weighted, coef + first),
            (power, energy, first),
        ):
            at = pl.ds(k, width)
            total = total + lax.dot_general(left[:, at], right[:, at], dims, preferred_element_type=jnp.float32)
        return total

    step = 2 * LANES
    total = jnp.zeros((ori, count), jnp.float32)
    if pieces > 1:
        for first in range(0, coef - coef % step, step):
            total = chunk(first, step, total)
    else:
        scores[...] = total

        @pl.loop(0, coef // step)
        def _(i):
            scores[...] = chunk(pl.multiple_of(i * step, step), step, scores[...])

        total = scores[...]
    if coef % step:
        total = chunk(coef - coef % step, coef % step, total)
    scores[...] = total
    top = jnp.max(total, axis=0, keepdims=True)
    expon = jnp.exp(total - top)
    index = me * ori + lax.broadcasted_iota(jnp.int32, total.shape, 0)
    begin = start[...]
    end = begin + length[...]
    end = jnp.where(end > all_orients, end - all_orients, end)
    stats[0:1, :] = top
    stats[1:2, :] = jnp.sum(expon, axis=0, keepdims=True)
    stats[2:3, :] = jnp.sum(jnp.where(index < begin, expon, 0.0), axis=0, keepdims=True)
    stats[3:4, :] = jnp.sum(jnp.where(index < end, expon, 0.0), axis=0, keepdims=True)


def running_body(scores, stats, expon_out, running_out, expon_pad, running_pad):
    ori, count = scores.shape
    top = stats[0:1, :]
    carry = jnp.zeros((1, count), jnp.float32)
    sub = lax.broadcasted_iota(jnp.int32, (8, count), 0)
    for o in range(0, ori, 8):
        value = jnp.exp(scores[pl.ds(o, 8), :] - top)
        total = value
        for step in (1, 2, 4):
            total = total + jnp.where(sub >= step, pltpu.roll(total, step, 0), 0.0)
        total = total + carry
        carry = total[7:8, :]
        expon_pad[pl.ds(o, 8), pl.ds(0, count)] = value
        running_pad[pl.ds(o, 8), pl.ds(0, count)] = total
    for o in range(0, ori, LANES):
        width = min(LANES, ori - o)
        for c in range(0, count, LANES):
            high = min(LANES, count - c)
            for pad, out in ((expon_pad, expon_out), (running_pad, running_out)):
                block = pad[pl.ds(o, LANES), pl.ds(c, LANES)].T
                out[pl.ds(c, high), pl.ds(o, width)] = block[:high, :width]


def final_body(near, far, thresholds, start, length, expon, running, *outs, all_orients):
    posterior, cumulative, evidence, mass = outs
    me = lax.axis_index("orient")
    half = near.shape[0] // 4
    tables = [near[pl.ds(4 * b, 4), :] for b in range(half)] + [far[pl.ds(4 * b, 4), :] for b in range(half)]
    top = tables[0][0:1, :]
    for table in tables[1:]:
        top = jnp.maximum(top, table[0:1, :])
    sums = jnp.zeros_like(tables[0])
    shifted = jnp.zeros_like(top)
    for b, table in enumerate(tables):
        scaled = table * jnp.exp(table[0:1, :] - top)
        sums = sums + scaled
        earlier = jnp.where((me ^ b) < me, 1.0, 0.0)
        shifted = shifted + earlier * scaled[1:2, :]
    total = sums[1:2, :]
    evidence[...] = top + jnp.log(total)
    fraction = thresholds[...].astype(jnp.float32) / 1024.0
    wraps = start[...] + length[...] > all_orients
    before = jnp.minimum(sums[2:3, :] / total, fraction)
    until = jnp.minimum(sums[3:4, :] / total, fraction)
    whole = jnp.where(wraps, jnp.minimum(1.0, fraction), 0.0)
    mass[...] = until - before + whole
    scale = column(jnp.exp(tables[0][0:1, :] - top) / total)
    shift = column(shifted / total)
    posterior[...] = expon[...] * scale
    cumulative[...] = running[...] * scale + shift


def call(body, limit, **kwargs):
    params = pltpu.CompilerParams(vmem_limit_bytes=limit)
    return pl.pallas_call(body, compiler_params=params, **kwargs)


def in_vmem(x):
    return pltpu.with_memory_space_constraint(x, pltpu.VMEM)


def in_hbm(x):
    return pltpu.with_memory_space_constraint(x, pltpu.HBM)


def on_device(particles, defocus, inv_noise, references, thresholds, range_start, range_len):
    n = lax.axis_size("orient")
    rows, feat = particles.shape
    coef = inv_noise.shape[0]
    ori = references.shape[0]
    count = n * rows
    all_orients = n * ori
    start = in_vmem(range_start.reshape(1, count))
    length = in_vmem(range_len.reshape(1, count))
    fraction = in_vmem(thresholds.reshape(1, count))
    f32, bf16 = jnp.float32, jnp.bfloat16

    def swap(x, even, odd):
        steps = (even, odd)
        parts = lax.axis_size("dom")
        pairs = [(i * parts + d, (i ^ steps[d % 2]) * parts + d) for i in range(n) for d in range(parts)]
        return lax.ppermute(x, ("orient", "dom"), pairs)

    packed = call(
        pack_body,
        2**21,
        out_shape=pltpu.VMEM((rows, feat + LANES), bf16),
        in_specs=[HBM, HBM],
        out_specs=VMEM,
        scratch_shapes=[pltpu.VMEM((1, rows), f32), pltpu.SemaphoreType.DMA((2,))],
    )(in_hbm(particles), in_hbm(defocus.reshape(1, rows)))

    half = n // 2
    offsets = [(0, 0)]
    if n == 8:
        pieces = [packed]
        for source, even, odd in ROUTE:
            pieces.append(swap(pieces[source], even, odd))
            offsets.append((offsets[source][0] ^ even, offsets[source][1] ^ odd))
    else:
        pieces = [lax.all_gather(packed, "orient", axis=0, tiled=True)]

    local, power = call(
        power_body,
        2**21,
        out_shape=(pltpu.VMEM((ori, feat), bf16), pltpu.VMEM((ori, coef), bf16)),
        in_specs=[HBM],
        out_specs=(VMEM, VMEM),
        scratch_shapes=[pltpu.SemaphoreType.DMA((9,))],
    )(in_hbm(references))

    room = 2**22 + 4 * count * (feat + LANES) + 3 * count * feat
    scores, stats = call(
        lambda *refs: score_body(*refs, pieces=len(pieces), offsets=offsets, all_orients=all_orients),
        room,
        out_shape=(pltpu.VMEM((ori, count), f32), pltpu.VMEM((4, count), f32)),
        in_specs=[VMEM] * (5 + len(pieces)),
        out_specs=(VMEM, VMEM),
        scratch_shapes=[
            pltpu.VMEM((count, feat) if len(pieces) > 1 else (8, LANES), f32),
            pltpu.VMEM((count, LANES), f32),
            pltpu.VMEM((count, feat), bf16),
            pltpu.VMEM((count, coef), bf16),
        ],
    )(start, length, in_vmem(inv_noise), in_vmem(local), in_vmem(power), *[in_vmem(p) for p in pieces])

    if n == 8:
        near = jnp.concatenate([stats] + [swap(stats, b, b) for b in range(1, half)], axis=0)
    else:
        near = stats
        b = 1
        while b < half:
            near = jnp.concatenate([near, swap(near, b, b)], axis=0)
            b *= 2
    far = swap(near, half, half)

    pad_ori = -(-ori // LANES) * LANES
    pad_count = -(-count // LANES) * LANES
    expon, running = call(
        running_body,
        2**23,
        out_shape=(pltpu.VMEM((count, ori), f32),) * 2,
        in_specs=[VMEM, VMEM],
        out_specs=(VMEM, VMEM),
        scratch_shapes=[pltpu.VMEM((pad_ori, pad_count), f32)] * 2,
    )(in_vmem(scores), in_vmem(stats))

    posterior, cumulative, evidence, mass = call(
        lambda *refs: final_body(*refs, all_orients=all_orients),
        2**23,
        out_shape=(jax.ShapeDtypeStruct((count, ori), f32),) * 2 + (jax.ShapeDtypeStruct((1, count), f32),) * 2,
        in_specs=[VMEM] * 7,
        out_specs=(VMEM,) * 4,
    )(in_vmem(near), in_vmem(far), fraction, start, length, in_vmem(expon), in_vmem(running))
    return posterior, cumulative, evidence.reshape(count), mass.reshape(count)


def solution(mesh):
    return jax.shard_map(
        on_device,
        mesh=mesh,
        in_specs=(
            P(("dom", "orient"), None),
            P(("dom", "orient")),
            P(),
            P(("dom", "orient"), None),
            P("dom"),
            P("dom"),
            P("dom"),
        ),
        out_specs=(P("dom", "orient"), P("dom", "orient"), P("dom"), P("dom")),
        check_vma=False,
    )
```

```python
import math

import jax
import jax.numpy as jnp
from jax import lax
from jax.experimental import pallas as pl
from jax.experimental.pallas import tpu as pltpu
from jax.sharding import PartitionSpec as P


LANES = 128
VMEM = pl.BlockSpec(memory_space=pltpu.VMEM)
HBM = pl.BlockSpec(memory_space=pltpu.HBM)


def minus_sine(x):
    turns = jnp.floor(x * (1.0 / math.pi) + 0.5)
    rest = x - turns * 3.1414794921875
    rest = rest - turns * 0.00011315941810607910156
    rest = rest - turns * 1.9841872589410058936e-09
    sq = rest * rest
    poly = sq * 2.6083159809786593541503e-06 - 0.0001981069071916863322258
    poly = poly * sq + 0.00833307858556509017944336
    poly = poly * sq - 0.166666597127914428710938
    value = rest + rest * (sq * poly)
    half = turns * 0.5
    return value * ((half - jnp.floor(half)) * 4.0 - 1.0)


def column(row):
    size = row.shape[1]
    down = lax.broadcasted_iota(jnp.int32, (size, size), 0)
    across = lax.broadcasted_iota(jnp.int32, (size, size), 1)
    return jnp.sum(jnp.where(down == across, row, 0.0), axis=1, keepdims=True)


def pack_body(particles, defocus, out, row, sems):
    feat = particles.shape[1]
    copy = pltpu.make_async_copy(particles, out.at[:, pl.ds(0, feat)], sems.at[0])
    fetch = pltpu.make_async_copy(defocus, row, sems.at[1])
    fetch.start()
    copy.start()
    fetch.wait()
    value = column(row[...])
    high = value.astype(jnp.bfloat16).astype(jnp.float32)
    mid = (value - high).astype(jnp.bfloat16).astype(jnp.float32)
    low = value - high - mid
    lane = lax.broadcasted_iota(jnp.int32, (value.shape[0], LANES), 1)
    parts = jnp.where(lane == 0, high, jnp.where(lane == 1, mid, jnp.where(lane == 2, low, 0.0)))
    out[:, pl.ds(feat, LANES)] = parts.astype(jnp.bfloat16)
    copy.wait()


def focus_of(piece, cut):
    bits = piece[:, pl.ds(2 * cut, LANES)].astype(jnp.float32)
    value = bits[:, 0:1] + bits[:, 1:2] + bits[:, 2:3]
    return jnp.broadcast_to(value, (value.shape[0], LANES))


def frequencies(k):
    col_pos = (lax.broadcasted_iota(jnp.int32, (1, LANES), 1) - 64).astype(jnp.float32)
    row_pos = jnp.asarray(k // 128).astype(jnp.float32)
    return math.pi * (row_pos * row_pos + col_pos * col_pos) / 16384.0


def weigh(real, imag, focus, noise_row, freq):
    ctf = minus_sine(focus * freq + 0.07)
    power = (ctf * ctf * noise_row).astype(jnp.bfloat16).astype(jnp.float32)
    return real.astype(jnp.float32) * ctf * noise_row, imag.astype(jnp.float32) * ctf * noise_row, -0.5 * power


def product(left, left_at, right):
    dims = (((1,), (1,)), ((), ()))
    return lax.dot_general(left[:, left_at], right, dims, preferred_element_type=jnp.float32)


def contract(total, references, power, stage, first, last, base):
    coef = power.shape[1]
    span = stage.shape[1] // 3
    for left, shift, block in ((references, 0, 0), (references, coef, 1), (power, 0, 2)):
        right = stage[:, pl.ds(block * span + first - base, last - first)]
        part = product(left, pl.ds(shift + first, last - first), right)
        total = part if total is None else total + part
    return total


def fill(stage, row, base, pieces, focuses, noise, k):
    span = stage.shape[1] // 3
    rows = pieces[0][0].shape[0]
    for i in range(0, len(pieces), 2):
        values = [
            weigh(piece[:, pl.ds(real, LANES)], piece[:, pl.ds(imag, LANES)], focus, noise[pl.ds(k, LANES)].reshape(1, LANES), frequencies(k))
            for (piece, real, imag), focus in zip(pieces[i : i + 2], focuses[i : i + 2])
        ]
        for block, pair in enumerate(zip(*values)):
            at = pl.ds(block * span + k - base, LANES)
            stage[pl.ds(row + i * rows, len(pair) * rows), at] = jnp.concatenate(pair, axis=0).astype(jnp.bfloat16)


def weigh_body(noise, *refs):
    pieces, stage = refs[:-1], refs[-1]
    coef = stage.shape[1] // 3
    focuses = [focus_of(piece, coef) for piece in pieces]
    for k in range(0, coef, LANES):
        fill(stage, 0, 0, [(piece, k, coef + k) for piece in pieces], focuses, noise, k)


def score_late_body(*refs, row, all_orients):
    start, length, noise, references, power = refs[:5]
    pieces = refs[6:-3]
    scores, stats, stage = refs[-3:]
    coef = power.shape[1]
    focuses = [focus_of(piece, coef) for piece in pieces]
    total = None
    for first in range(0, coef, 2 * LANES):
        last = min(first + 2 * LANES, coef)
        for k in range(first, last, LANES):
            fill(stage, row, 0, [(piece, k, coef + k) for piece in pieces], focuses, noise, k)
        total = contract(total, references, power, stage, first, last, 0)
    scores[...] = total
    statistics(total, start, length, stats, all_orients, pieces[0].shape[0])


def reorder(x, rows, me):
    count = x.shape[1]
    x = jnp.concatenate([x] * (LANES // count), axis=1)
    lane = lax.broadcasted_iota(jnp.int32, x.shape, 1)
    step = rows
    while step < count:
        swapped = jnp.where((lane & step) != 0, pltpu.roll(x, step, 1), pltpu.roll(x, LANES - step, 1))
        x = jnp.where((me & (step // rows)) != 0, swapped, x)
        step *= 2
    return x[:, :count]


def statistics(total, start, length, stats, all_orients, rows=None):
    me = lax.axis_index("orient")
    base = me * total.shape[0]
    begin = start[...]
    end = begin + length[...]
    end = jnp.where(end > all_orients, end - all_orients, end) - base
    begin = begin - base
    if rows:
        begin = reorder(begin, rows, me)
        end = reorder(end, rows, me)
    top = jnp.max(total, axis=0, keepdims=True)
    expon = jnp.exp(total - top)
    index = lax.broadcasted_iota(jnp.int32, total.shape, 0)
    table = jnp.concatenate(
        [
            top,
            jnp.sum(expon, axis=0, keepdims=True),
            jnp.sum(jnp.where(index < begin, expon, 0.0), axis=0, keepdims=True),
            jnp.sum(jnp.where(index < end, expon, 0.0), axis=0, keepdims=True),
        ],
        axis=0,
    )
    stats[...] = reorder(table, rows, me) if rows else table


def power_body(references, local, out, sems):
    rows, coef = out.shape
    step = -(-rows // (8 * sems.shape[0])) * 8
    spans = [pl.ds(r, min(step, rows - r)) for r in range(0, rows, step)]
    copies = [pltpu.make_async_copy(references.at[span], local.at[span], sems.at[i]) for i, span in enumerate(spans)]
    for copy in copies:
        copy.start()
    for span, copy in zip(spans, copies):
        copy.wait()
        for k in range(0, coef, LANES):
            real = local[span, pl.ds(k, LANES)].astype(jnp.float32)
            imag = local[span, pl.ds(coef + k, LANES)].astype(jnp.float32)
            out[span, pl.ds(k, LANES)] = (real * real + imag * imag).astype(jnp.bfloat16)


def score_body(start, length, noise, references, power, packed, scores, stats, stage, *, all_orients):
    coef = power.shape[1]
    step = 2 * LANES
    scores[...] = jnp.zeros(scores.shape, jnp.float32)

    def chunk(first, width):
        focus = focus_of(packed, coef)
        for k in range(0, width, LANES):
            noise_row = noise[pl.ds(first + k, LANES)].reshape(1, LANES)
            real = packed[:, pl.ds(first + k, LANES)]
            imag = packed[:, pl.ds(coef + first + k, LANES)]
            values = weigh(real, imag, focus, noise_row, frequencies(first + k))
            for block, value in enumerate(values):
                stage[:, pl.ds(block * step + k, LANES)] = value.astype(jnp.bfloat16)
        total = product(references, pl.ds(first, width), stage[:, pl.ds(0, width)])
        total = total + product(references, pl.ds(coef + first, width), stage[:, pl.ds(step, width)])
        scores[...] += total + product(power, pl.ds(first, width), stage[:, pl.ds(2 * step, width)])

    @pl.loop(0, coef // step)
    def _(i):
        chunk(pl.multiple_of(i * step, step), step)

    if coef % step:
        chunk(coef - coef % step, coef % step)
    statistics(scores[...], start, length, stats, all_orients)


def running_body(scores, stats, expon_out, running_out, expon_pad, running_pad, *, rows):
    ori, count = scores.shape
    me = lax.axis_index("orient")
    top = stats[0:1, :]
    if rows:
        top = reorder(top, rows, me)
    carry = jnp.zeros((1, count), jnp.float32)
    sub = lax.broadcasted_iota(jnp.int32, (8, count), 0)
    for o in range(0, ori, 8):
        value = jnp.exp(scores[pl.ds(o, 8), :] - top)
        total = value
        for step in (1, 2, 4):
            total = total + jnp.where(sub >= step, pltpu.roll(total, step, 0), 0.0)
        total = total + carry
        carry = total[7:8, :]
        expon_pad[pl.ds(o, 8), pl.ds(0, count)] = value
        running_pad[pl.ds(o, 8), pl.ds(0, count)] = total
    for o in range(0, ori, LANES):
        width = min(LANES, ori - o)
        for c in range(0, count, LANES):
            high = min(LANES, count - c)
            for pad, out in ((expon_pad, expon_out), (running_pad, running_out)):
                block = pad[pl.ds(o, LANES), pl.ds(c, LANES)].T
                if rows:
                    for b in range(high // rows):
                        place = pl.multiple_of((me ^ b) * rows, rows)
                        out[pl.ds(place, rows), pl.ds(o, width)] = block[b * rows : (b + 1) * rows, :width]
                else:
                    out[pl.ds(c, high), pl.ds(o, width)] = block[:high, :width]


def final_body(near, far, thresholds, start, length, expon, running, *outs, all_orients):
    posterior, cumulative, evidence, mass = outs
    me = lax.axis_index("orient")
    half = near.shape[0] // 4
    tables = [near[pl.ds(4 * b, 4), :] for b in range(half)] + [far[pl.ds(4 * b, 4), :] for b in range(half)]
    top = tables[0][0:1, :]
    for table in tables[1:]:
        top = jnp.maximum(top, table[0:1, :])
    sums = jnp.zeros_like(tables[0])
    shifted = jnp.zeros_like(top)
    for b, table in enumerate(tables):
        scaled = table * jnp.exp(table[0:1, :] - top)
        sums = sums + scaled
        earlier = jnp.where((me ^ b) < me, 1.0, 0.0)
        shifted = shifted + earlier * scaled[1:2, :]
    total = sums[1:2, :]
    evidence[...] = top + jnp.log(total)
    fraction = thresholds[...].astype(jnp.float32) / 1024.0
    wraps = start[...] + length[...] > all_orients
    before = jnp.minimum(sums[2:3, :] / total, fraction)
    until = jnp.minimum(sums[3:4, :] / total, fraction)
    whole = jnp.where(wraps, jnp.minimum(1.0, fraction), 0.0)
    mass[...] = until - before + whole
    scale = column(jnp.exp(tables[0][0:1, :] - top) / total)
    shift = column(shifted / total)
    posterior[...] = expon[...] * scale
    cumulative[...] = running[...] * scale + shift


def call(body, limit, **kwargs):
    params = pltpu.CompilerParams(vmem_limit_bytes=limit)
    return pl.pallas_call(body, compiler_params=params, **kwargs)


def in_vmem(x):
    return pltpu.with_memory_space_constraint(x, pltpu.VMEM)


def in_hbm(x):
    return pltpu.with_memory_space_constraint(x, pltpu.HBM)


def on_device(particles, defocus, inv_noise, references, thresholds, range_start, range_len):
    n = lax.axis_size("orient")
    rows, feat = particles.shape
    coef = inv_noise.shape[0]
    ori = references.shape[0]
    count = n * rows
    all_orients = n * ori
    start = in_vmem(range_start.reshape(1, count))
    length = in_vmem(range_len.reshape(1, count))
    fraction = in_vmem(thresholds.reshape(1, count))
    f32, bf16 = jnp.float32, jnp.bfloat16

    def swap(x, even, odd):
        steps = (even, odd)
        parts = lax.axis_size("dom")
        pairs = [(i * parts + d, (i ^ steps[d % 2]) * parts + d) for i in range(n) for d in range(parts)]
        return lax.ppermute(x, ("orient", "dom"), pairs)

    half = n // 2
    few = n == 8
    packed = call(
        pack_body,
        2**21,
        out_shape=pltpu.VMEM((rows, feat + LANES), bf16),
        in_specs=[HBM, HBM],
        out_specs=VMEM,
        scratch_shapes=[pltpu.VMEM((1, rows), f32), pltpu.SemaphoreType.DMA((2,))],
    )(in_hbm(particles), in_hbm(defocus.reshape(1, rows)))

    local, power = call(
        power_body,
        2**21,
        out_shape=(pltpu.VMEM((ori, feat), bf16), pltpu.VMEM((ori, coef), bf16)),
        in_specs=[HBM],
        out_specs=(VMEM, VMEM),
        scratch_shapes=[pltpu.SemaphoreType.DMA((9,))],
    )(in_hbm(references))
    noise = in_vmem(inv_noise)
    local, power = in_vmem(local), in_vmem(power)
    results = (pltpu.VMEM((ori, count), f32), pltpu.VMEM((4, count), f32))

    if few:
        pieces = {0: packed, half: swap(packed, half, half)}
        for source in (0, half):
            for b in range(half - 1, 0, -1):
                pieces[source ^ b] = swap(pieces[source], b, b)
        stage = pltpu.VMEM((count, 3 * coef), bf16)
        weighted = call(
            weigh_body, 2**22, out_shape=stage, in_specs=[VMEM] * (1 + half), out_specs=VMEM
        )(noise, *[in_vmem(pieces[b]) for b in range(half)])
        scores, stats, _ = call(
            lambda *refs: score_late_body(*refs, row=half * rows, all_orients=all_orients),
            2**23,
            out_shape=results + (stage,),
            in_specs=[VMEM] * (6 + half),
            out_specs=(VMEM,) * 3,
            input_output_aliases={5: 2},
        )(start, length, noise, local, power, in_vmem(weighted), *[in_vmem(pieces[b]) for b in range(half, n)])
    else:
        gathered = lax.all_gather(packed, "orient", axis=0, tiled=True)
        scores, stats = call(
            lambda *refs: score_body(*refs, all_orients=all_orients),
            2**24,
            out_shape=results,
            in_specs=[VMEM] * 6,
            out_specs=(VMEM, VMEM),
            scratch_shapes=[pltpu.VMEM((count, 6 * LANES), bf16)],
        )(start, length, noise, local, power, in_vmem(gathered))

    if few:
        near = jnp.concatenate([stats] + [swap(stats, b, b) for b in range(1, half)], axis=0)
    else:
        near = stats
        b = 1
        while b < half:
            near = jnp.concatenate([near, swap(near, b, b)], axis=0)
            b *= 2
    far = swap(near, half, half)

    pad_ori = -(-ori // LANES) * LANES
    pad_count = -(-count // LANES) * LANES
    expon, running = call(
        lambda *refs: running_body(*refs, rows=rows if few else None),
        2**23,
        out_shape=(pltpu.VMEM((count, ori), f32),) * 2,
        in_specs=[VMEM, VMEM],
        out_specs=(VMEM, VMEM),
        scratch_shapes=[pltpu.VMEM((pad_ori, pad_count), f32)] * 2,
    )(in_vmem(scores), in_vmem(stats))

    posterior, cumulative, evidence, mass = call(
        lambda *refs: final_body(*refs, all_orients=all_orients),
        2**23,
        out_shape=(jax.ShapeDtypeStruct((count, ori), f32),) * 2 + (jax.ShapeDtypeStruct((1, count), f32),) * 2,
        in_specs=[VMEM] * 7,
        out_specs=(VMEM,) * 4,
    )(in_vmem(near), in_vmem(far), fraction, start, length, in_vmem(expon), in_vmem(running))
    return posterior, cumulative, evidence.reshape(count), mass.reshape(count)


def solution(mesh):
    return jax.shard_map(
        on_device,
        mesh=mesh,
        in_specs=(
            P(("dom", "orient"), None),
            P(("dom", "orient")),
            P(),
            P(("dom", "orient"), None),
            P("dom"),
            P("dom"),
            P("dom"),
        ),
        out_specs=(P("dom", "orient"), P("dom", "orient"), P("dom"), P("dom")),
        check_vma=False,
    )
```

```python
import math

import jax
import jax.numpy as jnp
from jax import lax
from jax.experimental import pallas as pl
from jax.experimental.pallas import tpu as pltpu
from jax.sharding import PartitionSpec as P


LANES = 128
VMEM = pl.BlockSpec(memory_space=pltpu.VMEM)
HBM = pl.BlockSpec(memory_space=pltpu.HBM)


def minus_sine(x):
    turns = jnp.floor(x * (1.0 / math.pi) + 0.5)
    rest = x - turns * 3.1414794921875
    rest = rest - turns * 0.00011315941810607910156
    rest = rest - turns * 1.9841872589410058936e-09
    sq = rest * rest
    poly = sq * 2.6083159809786593541503e-06 - 0.0001981069071916863322258
    poly = poly * sq + 0.00833307858556509017944336
    poly = poly * sq - 0.166666597127914428710938
    value = rest + rest * (sq * poly)
    half = turns * 0.5
    return value * ((half - jnp.floor(half)) * 4.0 - 1.0)


def column(row):
    size = row.shape[1]
    down = lax.broadcasted_iota(jnp.int32, (size, size), 0)
    across = lax.broadcasted_iota(jnp.int32, (size, size), 1)
    return jnp.sum(jnp.where(down == across, row, 0.0), axis=1, keepdims=True)


def pack_body(particles, defocus, out, row, sems):
    feat = particles.shape[1]
    width = -(-feat // (LANES * (sems.shape[0] - 1))) * LANES
    spans = [pl.ds(k, min(width, feat - k)) for k in range(0, feat, width)]
    copies = [pltpu.make_async_copy(particles.at[:, span], out.at[:, span], sems.at[i + 1]) for i, span in enumerate(spans)]
    fetch = pltpu.make_async_copy(defocus, row, sems.at[0])
    fetch.start()
    for copy in copies:
        copy.start()
    fetch.wait()
    value = column(row[...])
    high = value.astype(jnp.bfloat16).astype(jnp.float32)
    mid = (value - high).astype(jnp.bfloat16).astype(jnp.float32)
    low = value - high - mid
    lane = lax.broadcasted_iota(jnp.int32, (value.shape[0], LANES), 1)
    parts = jnp.where(lane == 0, high, jnp.where(lane == 1, mid, jnp.where(lane == 2, low, 0.0)))
    out[:, pl.ds(feat, LANES)] = parts.astype(jnp.bfloat16)
    for copy in copies:
        copy.wait()


def focus_of(piece, cut):
    bits = piece[:, pl.ds(2 * cut, LANES)].astype(jnp.float32)
    value = bits[:, 0:1] + bits[:, 1:2] + bits[:, 2:3]
    return jnp.broadcast_to(value, (value.shape[0], LANES))


def frequencies(k):
    col_pos = (lax.broadcasted_iota(jnp.int32, (1, LANES), 1) - 64).astype(jnp.float32)
    row_pos = jnp.asarray(k // 128).astype(jnp.float32)
    return math.pi * (row_pos * row_pos + col_pos * col_pos) / 16384.0


def weigh(real, imag, focus, noise_row, freq):
    ctf = minus_sine(focus * freq + 0.07)
    power = (ctf * ctf * noise_row).astype(jnp.bfloat16).astype(jnp.float32)
    return real.astype(jnp.float32) * ctf * noise_row, imag.astype(jnp.float32) * ctf * noise_row, -0.5 * power


def product(left, left_at, right):
    dims = (((1,), (1,)), ((), ()))
    return lax.dot_general(left[:, left_at], right, dims, preferred_element_type=jnp.float32)


def contract(total, references, power, stage, first, last, base):
    coef = power.shape[1]
    span = stage.shape[1] // 3
    for left, shift, block in ((references, 0, 0), (references, coef, 1), (power, 0, 2)):
        right = stage[:, pl.ds(block * span + first - base, last - first)]
        part = product(left, pl.ds(shift + first, last - first), right)
        total = part if total is None else total + part
    return total


def fill(stage, row, base, pieces, focuses, noise, k):
    span = stage.shape[1] // 3
    rows = pieces[0][0].shape[0]
    for i in range(0, len(pieces), 2):
        values = [
            weigh(piece[:, pl.ds(real, LANES)], piece[:, pl.ds(imag, LANES)], focus, noise[pl.ds(k, LANES)].reshape(1, LANES), frequencies(k))
            for (piece, real, imag), focus in zip(pieces[i : i + 2], focuses[i : i + 2])
        ]
        for block, pair in enumerate(zip(*values)):
            at = pl.ds(block * span + k - base, LANES)
            stage[pl.ds(row + i * rows, len(pair) * rows), at] = jnp.concatenate(pair, axis=0).astype(jnp.bfloat16)


def weigh_body(noise, *refs):
    pieces, stage = refs[:-1], refs[-1]
    coef = stage.shape[1] // 3
    focuses = [focus_of(piece, coef) for piece in pieces]
    for k in range(0, coef, LANES):
        fill(stage, 0, 0, [(piece, k, coef + k) for piece in pieces], focuses, noise, k)


def score_late_body(*refs, row, all_orients):
    start, length, noise, references, power = refs[:5]
    pieces = refs[6:-3]
    scores, stats, stage = refs[-3:]
    coef = power.shape[1]
    focuses = [focus_of(piece, coef) for piece in pieces]
    total = None
    for first in range(0, coef, 2 * LANES):
        last = min(first + 2 * LANES, coef)
        for k in range(first, last, LANES):
            fill(stage, row, 0, [(piece, k, coef + k) for piece in pieces], focuses, noise, k)
        total = contract(total, references, power, stage, first, last, 0)
    scores[...] = total
    statistics(total, start, length, stats, all_orients, pieces[0].shape[0])


def reorder(x, rows, me):
    count = x.shape[1]
    x = jnp.concatenate([x] * (LANES // count), axis=1)
    lane = lax.broadcasted_iota(jnp.int32, x.shape, 1)
    step = rows
    while step < count:
        swapped = jnp.where((lane & step) != 0, pltpu.roll(x, step, 1), pltpu.roll(x, LANES - step, 1))
        x = jnp.where((me & (step // rows)) != 0, swapped, x)
        step *= 2
    return x[:, :count]


def statistics(total, start, length, stats, all_orients, rows=None):
    me = lax.axis_index("orient")
    base = me * total.shape[0]
    begin = start[...]
    end = begin + length[...]
    end = jnp.where(end > all_orients, end - all_orients, end) - base
    begin = begin - base
    if rows:
        begin = reorder(begin, rows, me)
        end = reorder(end, rows, me)
    top = jnp.max(total, axis=0, keepdims=True)
    expon = jnp.exp(total - top)
    index = lax.broadcasted_iota(jnp.int32, total.shape, 0)
    table = jnp.concatenate(
        [
            top,
            jnp.sum(expon, axis=0, keepdims=True),
            jnp.sum(jnp.where(index < begin, expon, 0.0), axis=0, keepdims=True),
            jnp.sum(jnp.where(index < end, expon, 0.0), axis=0, keepdims=True),
        ],
        axis=0,
    )
    stats[...] = reorder(table, rows, me) if rows else table


def power_body(references, local, out, sems):
    rows, coef = out.shape
    step = -(-rows // (8 * sems.shape[0])) * 8
    spans = [pl.ds(r, min(step, rows - r)) for r in range(0, rows, step)]
    copies = [pltpu.make_async_copy(references.at[span], local.at[span], sems.at[i]) for i, span in enumerate(spans)]
    for copy in copies:
        copy.start()
    for span, copy in zip(spans, copies):
        copy.wait()
        for k in range(0, coef, LANES):
            real = local[span, pl.ds(k, LANES)].astype(jnp.float32)
            imag = local[span, pl.ds(coef + k, LANES)].astype(jnp.float32)
            out[span, pl.ds(k, LANES)] = (real * real + imag * imag).astype(jnp.bfloat16)


def score_body(start, length, noise, references, power, packed, scores, stats, stage, *, all_orients):
    coef = power.shape[1]
    step = 2 * LANES
    scores[...] = jnp.zeros(scores.shape, jnp.float32)

    def chunk(first, width):
        focus = focus_of(packed, coef)
        for k in range(0, width, LANES):
            noise_row = noise[pl.ds(first + k, LANES)].reshape(1, LANES)
            real = packed[:, pl.ds(first + k, LANES)]
            imag = packed[:, pl.ds(coef + first + k, LANES)]
            values = weigh(real, imag, focus, noise_row, frequencies(first + k))
            for block, value in enumerate(values):
                stage[:, pl.ds(block * step + k, LANES)] = value.astype(jnp.bfloat16)
        total = product(references, pl.ds(first, width), stage[:, pl.ds(0, width)])
        total = total + product(references, pl.ds(coef + first, width), stage[:, pl.ds(step, width)])
        scores[...] += total + product(power, pl.ds(first, width), stage[:, pl.ds(2 * step, width)])

    @pl.loop(0, coef // step)
    def _(i):
        chunk(pl.multiple_of(i * step, step), step)

    if coef % step:
        chunk(coef - coef % step, coef % step)
    statistics(scores[...], start, length, stats, all_orients)


def running_body(scores, stats, expon_out, running_out, expon_pad, running_pad, *, rows):
    ori, count = scores.shape
    me = lax.axis_index("orient")
    top = stats[0:1, :]
    if rows:
        top = reorder(top, rows, me)
    carry = jnp.zeros((1, count), jnp.float32)
    sub = lax.broadcasted_iota(jnp.int32, (8, count), 0)
    for o in range(0, ori, 8):
        value = jnp.exp(scores[pl.ds(o, 8), :] - top)
        total = value
        for step in (1, 2, 4):
            total = total + jnp.where(sub >= step, pltpu.roll(total, step, 0), 0.0)
        total = total + carry
        carry = total[7:8, :]
        expon_pad[pl.ds(o, 8), pl.ds(0, count)] = value
        running_pad[pl.ds(o, 8), pl.ds(0, count)] = total
    for o in range(0, ori, LANES):
        width = min(LANES, ori - o)
        for c in range(0, count, LANES):
            high = min(LANES, count - c)
            for pad, out in ((expon_pad, expon_out), (running_pad, running_out)):
                block = pad[pl.ds(o, LANES), pl.ds(c, LANES)].T
                if rows:
                    for b in range(high // rows):
                        place = pl.multiple_of((me ^ b) * rows, rows)
                        out[pl.ds(place, rows), pl.ds(o, width)] = block[b * rows : (b + 1) * rows, :width]
                else:
                    out[pl.ds(c, high), pl.ds(o, width)] = block[:high, :width]


def final_body(near, far, thresholds, start, length, expon, running, *outs, all_orients):
    posterior, cumulative, evidence, mass = outs
    me = lax.axis_index("orient")
    half = near.shape[0] // 4
    tables = [near[pl.ds(4 * b, 4), :] for b in range(half)] + [far[pl.ds(4 * b, 4), :] for b in range(half)]
    top = tables[0][0:1, :]
    for table in tables[1:]:
        top = jnp.maximum(top, table[0:1, :])
    sums = jnp.zeros_like(tables[0])
    shifted = jnp.zeros_like(top)
    for b, table in enumerate(tables):
        scaled = table * jnp.exp(table[0:1, :] - top)
        sums = sums + scaled
        earlier = jnp.where((me ^ b) < me, 1.0, 0.0)
        shifted = shifted + earlier * scaled[1:2, :]
    total = sums[1:2, :]
    evidence[...] = top + jnp.log(total)
    fraction = thresholds[...].astype(jnp.float32) / 1024.0
    wraps = start[...] + length[...] > all_orients
    before = jnp.minimum(sums[2:3, :] / total, fraction)
    until = jnp.minimum(sums[3:4, :] / total, fraction)
    whole = jnp.where(wraps, jnp.minimum(1.0, fraction), 0.0)
    mass[...] = until - before + whole
    scale = column(jnp.exp(tables[0][0:1, :] - top) / total)
    shift = column(shifted / total)
    posterior[...] = expon[...] * scale
    cumulative[...] = running[...] * scale + shift


def call(body, limit, **kwargs):
    params = pltpu.CompilerParams(vmem_limit_bytes=limit)
    return pl.pallas_call(body, compiler_params=params, **kwargs)


def in_vmem(x):
    return pltpu.with_memory_space_constraint(x, pltpu.VMEM)


def in_hbm(x):
    return pltpu.with_memory_space_constraint(x, pltpu.HBM)


def on_device(particles, defocus, inv_noise, references, thresholds, range_start, range_len):
    n = lax.axis_size("orient")
    rows, feat = particles.shape
    coef = inv_noise.shape[0]
    ori = references.shape[0]
    count = n * rows
    all_orients = n * ori
    start = in_vmem(range_start.reshape(1, count))
    length = in_vmem(range_len.reshape(1, count))
    fraction = in_vmem(thresholds.reshape(1, count))
    f32, bf16 = jnp.float32, jnp.bfloat16

    def swap(x, even, odd):
        steps = (even, odd)
        parts = lax.axis_size("dom")
        pairs = [(i * parts + d, (i ^ steps[d % 2]) * parts + d) for i in range(n) for d in range(parts)]
        return lax.ppermute(x, ("orient", "dom"), pairs)

    half = n // 2
    few = n == 8
    packed = call(
        pack_body,
        2**21,
        out_shape=pltpu.VMEM((rows, feat + LANES), bf16),
        in_specs=[HBM, HBM],
        out_specs=VMEM,
        scratch_shapes=[pltpu.VMEM((1, rows), f32), pltpu.SemaphoreType.DMA((7,))],
    )(in_hbm(particles), in_hbm(defocus.reshape(1, rows)))

    local, power = call(
        power_body,
        2**21,
        out_shape=(pltpu.VMEM((ori, feat), bf16), pltpu.VMEM((ori, coef), bf16)),
        in_specs=[HBM],
        out_specs=(VMEM, VMEM),
        scratch_shapes=[pltpu.SemaphoreType.DMA((9,))],
    )(in_hbm(references))
    noise = in_vmem(inv_noise)
    local, power = in_vmem(local), in_vmem(power)
    results = (pltpu.VMEM((ori, count), f32), pltpu.VMEM((4, count), f32))

    if few:
        pieces = {0: packed, half: swap(packed, half, half)}
        for source in (0, half):
            for b in range(half - 1, 0, -1):
                pieces[source ^ b] = swap(pieces[source], b, b)
        stage = pltpu.VMEM((count, 3 * coef), bf16)
        weighted = call(
            weigh_body, 2**22, out_shape=stage, in_specs=[VMEM] * (1 + half), out_specs=VMEM
        )(noise, *[in_vmem(pieces[b]) for b in range(half)])
        scores, stats, _ = call(
            lambda *refs: score_late_body(*refs, row=half * rows, all_orients=all_orients),
            2**23,
            out_shape=results + (stage,),
            in_specs=[VMEM] * (6 + half),
            out_specs=(VMEM,) * 3,
            input_output_aliases={5: 2},
        )(start, length, noise, local, power, in_vmem(weighted), *[in_vmem(pieces[b]) for b in range(half, n)])
    else:
        gathered = lax.all_gather(packed, "orient", axis=0, tiled=True)
        scores, stats = call(
            lambda *refs: score_body(*refs, all_orients=all_orients),
            2**24,
            out_shape=results,
            in_specs=[VMEM] * 6,
            out_specs=(VMEM, VMEM),
            scratch_shapes=[pltpu.VMEM((count, 6 * LANES), bf16)],
        )(start, length, noise, local, power, in_vmem(gathered))

    if few:
        near = jnp.concatenate([stats] + [swap(stats, b, b) for b in range(1, half)], axis=0)
    else:
        near = stats
        b = 1
        while b < half:
            near = jnp.concatenate([near, swap(near, b, b)], axis=0)
            b *= 2
    far = swap(near, half, half)

    pad_ori = -(-ori // LANES) * LANES
    pad_count = -(-count // LANES) * LANES
    expon, running = call(
        lambda *refs: running_body(*refs, rows=rows if few else None),
        2**23,
        out_shape=(pltpu.VMEM((count, ori), f32),) * 2,
        in_specs=[VMEM, VMEM],
        out_specs=(VMEM, VMEM),
        scratch_shapes=[pltpu.VMEM((pad_ori, pad_count), f32)] * 2,
    )(in_vmem(scores), in_vmem(stats))

    posterior, cumulative, evidence, mass = call(
        lambda *refs: final_body(*refs, all_orients=all_orients),
        2**23,
        out_shape=(jax.ShapeDtypeStruct((count, ori), f32),) * 2 + (jax.ShapeDtypeStruct((1, count), f32),) * 2,
        in_specs=[VMEM] * 7,
        out_specs=(VMEM,) * 4,
    )(in_vmem(near), in_vmem(far), fraction, start, length, in_vmem(expon), in_vmem(running))
    return posterior, cumulative, evidence.reshape(count), mass.reshape(count)


def solution(mesh):
    return jax.shard_map(
        on_device,
        mesh=mesh,
        in_specs=(
            P(("dom", "orient"), None),
            P(("dom", "orient")),
            P(),
            P(("dom", "orient"), None),
            P("dom"),
            P("dom"),
            P("dom"),
        ),
        out_specs=(P("dom", "orient"), P("dom", "orient"), P("dom"), P("dom")),
        check_vma=False,
    )
```
